32 devices in a mesh: seq: 8 (over z, y), head: 4 (over x, core).
Axes of the slice: x: 2, y: 2, z: 4, core: 2. Of those that a mesh axis runs over, the one named last changes fastest.
Arguments:
- queries: float32 [1024, 8192], P('seq', 'head'), may hold values from -48 to 48
- prefix_keys: float32 [5120, 512], P('seq', 'head'), may hold values from -5 to 5
- prefix_value_rows: float32 [5120, 512], P('seq', 'head'), may hold values from -6 to 6
- response_keys: float32 [1024, 512], P('seq', 'head'), may hold values from -6 to 6
- response_values: float32 [1024, 512], P('seq', 'head'), may hold values from -6 to 6
- out_grad: float32 [1024, 8192], P('seq', 'head'), may hold values from -6 to 6
- lengths: int32 [8], P('seq'), may hold values from 32 to 128
Outputs:
- grad_queries: float32 [1024, 8192], P(('seq', 'head'))
- grad_prefix_keys: float32 [5120, 512], P('seq', 'head')
- grad_prefix_values: float32 [5120, 512], P('seq', 'head')
- grad_resp_keys: float32 [1024, 512], P('seq', 'head')
- grad_resp_values: float32 [1024, 512], P('seq', 'head')
The draws below stay inside these ranges and needn't reach their ends.
All inputs are finite; a program needn't handle non-finite values.
Results may differ from the reference program's by a relative error of at most 0.0003.
Values sent between devices are 32-bit elements; how exact they have to be, the bound alone decides.
A program may use at most 128 MiB of HBM per device.

```python
import jax
import jax.numpy as jnp
from jax import lax

QUERY_HEAD_COUNT = 64
KEY_VALUE_HEADS = 4
HEAD_SIZE = 128
BLOCK_PREFIX = 640
R_DEV = 128
WINDOW = 3
PREFIX_TOKENS = 5120
RESPONSE_SLOTS = 1024
N_SEQ = 8


def joint_draw(key):
    random_key_for_keys = jax.random.fold_in(key, 101)
    key_query = jax.random.fold_in(key, 202)
    key_matrix = jnp.clip(jax.random.normal(random_key_for_keys, (N_SEQ, BLOCK_PREFIX, KEY_VALUE_HEADS, HEAD_SIZE), jnp.float32), -4.0, 4.0)
    query_matrix = jnp.clip(jax.random.normal(key_query, (N_SEQ, R_DEV, QUERY_HEAD_COUNT, HEAD_SIZE), jnp.float32), -4.0, 4.0)
    return (key_matrix.reshape(PREFIX_TOKENS, KEY_VALUE_HEADS * HEAD_SIZE), query_matrix.reshape(RESPONSE_SLOTS, QUERY_HEAD_COUNT * HEAD_SIZE))


def draw_queries(key, part):
    return joint_draw(key)[1]


def draw_prefix_keys(key, part):
    return joint_draw(key)[0]


def set_ends(entries, key, low, high):
    place = [jax.random.randint(jax.random.fold_in(key, axis), (), 0, length) for axis, length in enumerate(entries.shape)]
    longest = entries.shape.index(max(entries.shape))
    next_to = place[:longest] + [(place[longest] + 1) % entries.shape[longest]] + place[longest + 1:]
    return entries.at[tuple(place)].set(low).at[tuple(next_to)].set(high)


def shard_levels(stream_key, dims, pieces, low, high):
    def one(position, shards_of):
        draws = jax.random.uniform(jax.random.fold_in(jax.random.fold_in(stream_key, 6), position), (shards_of,), jnp.float32, low / len(pieces), high / len(pieces))
        return jnp.repeat(jnp.exp(draws), dims[position] // shards_of).reshape((-1,) + (1,) * (len(dims) - position - 1))

    factor_of = one(*pieces[0])
    for cut in pieces[1:]:
        factor_of = factor_of * one(*cut)
    return factor_of


def bell_draw(stream_key, dims, width, bound, split=(), held_as=jnp.bfloat16):
    entries = jax.random.normal(stream_key, dims, jnp.float32) * width
    if len(split) > 0:
        entries = shard_levels(stream_key, dims, split, -0.22, 0.18) * entries
    return jnp.clip(entries, min=-bound, max=bound).astype(held_as)


def setup_inputs(seed: int = 0) -> dict:
    key_of = jax.random.split(jax.random.key(seed), 8)
    return {
        "queries": draw_queries(jax.random.fold_in(key_of[7], 71), 0),
        "prefix_keys": draw_prefix_keys(jax.random.fold_in(key_of[7], 71), 0),
        "prefix_value_rows": bell_draw(key_of[2], (PREFIX_TOKENS, KEY_VALUE_HEADS * HEAD_SIZE), 1.0, 6.0, ((0, 8), (1, 4)), jnp.float32),
        "response_keys": bell_draw(key_of[3], (RESPONSE_SLOTS, KEY_VALUE_HEADS * HEAD_SIZE), 1.0, 6.0, ((0, 8), (1, 4)), jnp.float32),
        "response_values": bell_draw(key_of[4], (RESPONSE_SLOTS, KEY_VALUE_HEADS * HEAD_SIZE), 1.0, 6.0, ((0, 8), (1, 4)), jnp.float32),
        "out_grad": bell_draw(key_of[5], (RESPONSE_SLOTS, QUERY_HEAD_COUNT * HEAD_SIZE), 1.0, 6.0, ((0, 8), (1, 4)), jnp.float32),
        "lengths": set_ends(jax.random.randint(key_of[6], (N_SEQ,), max(4, R_DEV // 4), R_DEV + 1), jax.random.fold_in(key_of[6], 1), max(4, R_DEV // 4), R_DEV).astype(jnp.int32),
    }


def attend(query_row_block, visible_key_rows, visible_value_rows, local_block_keys, local_block_values, length):
    row_count = query_row_block.shape[0]
    group_size = QUERY_HEAD_COUNT // KEY_VALUE_HEADS
    prefix_length = visible_key_rows.shape[0]
    query_block = query_row_block.reshape(row_count, KEY_VALUE_HEADS, group_size, HEAD_SIZE)
    key_matrix = jnp.concatenate([visible_key_rows, local_block_keys], axis=0).reshape(prefix_length + row_count, KEY_VALUE_HEADS, HEAD_SIZE)
    value_matrix = jnp.concatenate([visible_value_rows, local_block_values], axis=0).reshape(prefix_length + row_count, KEY_VALUE_HEADS, HEAD_SIZE)
    scores = jnp.einsum('rkgd,skd->kgrs', query_block, key_matrix, precision=lax.Precision.HIGHEST) * HEAD_SIZE ** (-0.5)
    slot = jnp.arange(prefix_length + row_count, dtype=jnp.int32) - prefix_length
    token = jnp.arange(row_count, dtype=jnp.int32)
    visible = (slot[None, :] < 0) | (slot[None, :] <= token[:, None]) & (slot[None, :] < length)
    scores = jnp.where(visible[None, None], scores, -1e+30)
    probs = jax.nn.softmax(scores, axis=-1)
    result = jnp.einsum('kgrs,skd->rkgd', probs, value_matrix, precision=lax.Precision.HIGHEST)
    return result.reshape(row_count, QUERY_HEAD_COUNT * HEAD_SIZE)

def reference(queries, prefix_keys, prefix_value_rows, response_keys, response_values, out_grad, lengths):
    window_width = KEY_VALUE_HEADS * HEAD_SIZE
    q_blocks = queries.reshape(N_SEQ, R_DEV, QUERY_HEAD_COUNT * HEAD_SIZE)
    g_blocks = out_grad.reshape(N_SEQ, R_DEV, QUERY_HEAD_COUNT * HEAD_SIZE)
    kp_blocks = prefix_keys.reshape(N_SEQ, BLOCK_PREFIX, window_width)
    vp_blocks = prefix_value_rows.reshape(N_SEQ, BLOCK_PREFIX, window_width)
    kr_blocks = response_keys.reshape(N_SEQ, R_DEV, window_width)
    vr_blocks = response_values.reshape(N_SEQ, R_DEV, window_width)

    def one_response(index):
        picks = (index + jnp.arange(WINDOW, dtype=jnp.int32)) % N_SEQ
        visible_key_rows = jnp.take(kp_blocks, picks, axis=0).reshape(WINDOW * BLOCK_PREFIX, window_width)
        visible_value_rows = jnp.take(vp_blocks, picks, axis=0).reshape(WINDOW * BLOCK_PREFIX, window_width)
        length = lengths[index]
        valid = (jnp.arange(R_DEV, dtype=jnp.int32) < length).astype(jnp.float32)

        def forward(a, b, c, d, e):
            return attend(a, b, c, d, e, length)
        _, pullback = jax.vjp(forward, q_blocks[index], visible_key_rows, visible_value_rows, kr_blocks[index], vr_blocks[index])
        dq, dkw, dvw, dkr, dvr = pullback(g_blocks[index] * valid[:, None])
        return (dq, dkw.reshape(WINDOW, BLOCK_PREFIX, window_width), dvw.reshape(WINDOW, BLOCK_PREFIX, window_width), dkr, dvr)
    dq, dkw, dvw, dkr, dvr = lax.map(one_response, jnp.arange(N_SEQ, dtype=jnp.int32))
    grad_k = dkw[:, 0]
    grad_v = dvw[:, 0]
    for offset in range(1, WINDOW):
        grad_k = grad_k + jnp.roll(dkw[:, offset], offset, axis=0)
        grad_v = grad_v + jnp.roll(dvw[:, offset], offset, axis=0)
    return (dq.reshape(RESPONSE_SLOTS, QUERY_HEAD_COUNT * HEAD_SIZE), grad_k.reshape(PREFIX_TOKENS, window_width), grad_v.reshape(PREFIX_TOKENS, window_width), dkr.reshape(RESPONSE_SLOTS, window_width), dvr.reshape(RESPONSE_SLOTS, window_width))
```

```python
import functools
import math

import jax
import jax.numpy as jnp
from jax import lax
from jax.experimental import pallas as pl
from jax.experimental.pallas import tpu as pltpu
from jax.sharding import PartitionSpec as P

HEAD_SIZE = 128
WINDOW = 3
D = HEAD_SIZE
MESH = pl.DeviceIdType.MESH
F32, BF16 = jnp.float32, jnp.bfloat16
SUB = 128
STEP = 4


def split(x):
    hi = x.astype(BF16)
    lo = (x - hi.astype(F32)).astype(BF16)
    return hi, lo


def dot(a, b):
    return jnp.dot(a, b, preferred_element_type=F32)


def kernel(
    n_seq, n_head,
    length_ref, q_hbm, pk_ref, pv_ref, rk_ref, rv_ref, g_hbm,
    gq_ref, gpk_ref, gpv_ref, grk_ref, grv_ref,
    q_ref, g_ref, kv0, kv1, kv2, kvr, kc, vc, kt, qt, gt, qr, gr, s_ref, dp_ref, m_ref, l_ref, d_ref,
    pcat, dcat, dk_acc, dv_acc, dqt, dqs, ry, rz,
    in_z_send, in_z_recv, in_y_send, in_y_recv,
    out_z_send, out_z_recv, out_y_send, out_y_recv,
    q_send, q_recv, q_local, load_sem,
):
    rows = q_hbm.shape[0]
    heads = q_hbm.shape[1] // D
    pairs = heads // 2
    block = pk_ref.shape[0]
    parts = block // SUB
    lead = block + rows
    cut = (parts + 1) // 2
    front_size, last_at, last_size = cut * SUB, cut * SUB, block - cut * SUB
    off1, off2 = lead, lead + block
    factor = D ** (-0.5)
    seq = lax.axis_index("seq")
    head = lax.axis_index("head")
    even = lax.rem(seq, 2) == 0
    odd = jnp.logical_not(even)
    partner = seq + 1 - 2 * lax.rem(seq, 2)
    below = lax.rem(seq + n_seq - 2, n_seq)
    above = lax.rem(seq + 2, n_seq)

    barrier = pltpu.get_barrier_semaphore()
    for other in (partner, below, above):
        pl.semaphore_signal(barrier, inc=1, device_id=(other, head), device_id_type=MESH)
    for step in range(1, n_head):
        pl.semaphore_signal(
            barrier, inc=1, device_id=(seq, lax.rem(head + step, n_head)), device_id_type=MESH
        )
    loads = [
        pltpu.make_async_copy(src, dst, load_sem.at[i])
        for i, (src, dst) in enumerate(
            (
                (pk_ref, kv0.at[0]),
                (pv_ref, kv0.at[1]),
                (rk_ref, kvr.at[0]),
                (rv_ref, kvr.at[1]),
                (q_hbm, q_ref),
                (g_hbm, g_ref),
            )
        )
    ]
    for load in loads:
        load.start()
    pl.semaphore_wait(barrier, 3 + n_head - 1)

    def remote(src, dst, send, recv, to):
        return pltpu.make_async_remote_copy(
            src_ref=src, dst_ref=dst, send_sem=send, recv_sem=recv,
            device_id=to, device_id_type=MESH,
        )

    own = (pk_ref, pv_ref)

    def piece(i):
        return pl.ds(i * SUB, SUB)

    def in_z(i, t):
        return remote(own[t].at[piece(i)], kv2.at[t, piece(i)], in_z_send.at[i, t], in_z_recv.at[i, t], (below, head))

    def in_y_own(i, t):
        return remote(own[t].at[piece(i)], kv1.at[t, piece(i)], in_y_send.at[i, t], in_y_recv.at[i, t], (partner, head))

    def in_y_pass(i, t):
        return remote(kv2.at[t, piece(i)], kv1.at[t, piece(i)], in_y_send.at[i, t], in_y_recv.at[i, t], (partner, head))

    pieces = [(i, t) for t in range(2) for i in range(parts)]
    for i, t in pieces:
        in_z(i, t).start()

    @pl.when(odd)
    def _():
        for i, t in pieces:
            in_y_own(i, t).start()

    def relay(t, some):
        for i in some:
            in_z(i, t).wait_recv()

            @pl.when(even)
            def _():
                in_y_pass(i, t).start()

    def arrive(t, some):
        for i in some:
            in_y_own(i, t).wait_recv()

    def place_keys(keys, first, offset, size):
        for start in range(0, size, SUB):
            here = pl.ds(offset + start, SUB)
            k = keys[pl.ds(first + start, SUB), :]
            hi, lo = split(k)
            kc[here, 0:D] = hi
            kc[here, D : 2 * D] = lo
            kc[here, 2 * D : 3 * D] = hi
            hi, lo = split(k.T)
            kt[0:D, here] = hi
            kt[D : 2 * D, here] = lo

    def place_values(values, first, offset, size):
        for start in range(0, size, SUB):
            here = pl.ds(offset + start, SUB)
            hi, lo = split(values[pl.ds(first + start, SUB), :])
            vc[here, 0:D] = hi
            vc[here, D : 2 * D] = lo
            vc[here, 2 * D : 3 * D] = hi

    for load in loads[:4]:
        load.wait()
    place_keys(kv0.at[0], 0, 0, block)
    place_values(kv0.at[1], 0, 0, block)
    place_keys(kvr.at[0], 0, block, rows)
    place_values(kvr.at[1], 0, block, rows)
    for load in loads[4:]:
        load.wait()

    length = length_ref[0]
    token = lax.broadcasted_iota(jnp.int32, (rows, 1), 0)
    live = token < length
    for h in range(heads):
        cols = pl.ds(h * D, D)
        pair, half = h // 2, h % 2
        lanes = pl.ds(half * rows, rows)
        q = q_ref[:, cols]
        g = jnp.where(live, g_ref[:, cols], 0.0)
        for x, wide, tall, scale in (
            (q, qr, qt, factor * math.log2(math.e)),
            (g, gr, gt, 1.0),
        ):
            hi, lo = split((x * scale).T)
            tall[pair, 0:D, lanes] = hi
            tall[pair, D : 2 * D, lanes] = hi
            tall[pair, 2 * D : 3 * D, lanes] = lo
            hi, lo = split(x * factor) if wide is qr else split(x)
            for copy in range(2):
                at_rows = pl.ds(copy * 2 * rows + half * rows, rows)
                wide[pair, at_rows, 0:D] = hi
                wide[pair, at_rows, D : 2 * D] = lo

    tile = (SUB // 8, 8, 2 * rows)

    def lead_products(pair):
        s = dot(kc[pl.ds(0, lead), :], qt[pair])
        slot = lax.broadcasted_iota(jnp.int32, (rows, 2 * rows), 0)
        lane = lax.broadcasted_iota(jnp.int32, (rows, 2 * rows), 1)
        query = jnp.where(lane >= rows, lane - rows, lane)
        visible = (slot <= query) & (slot < length)
        s_ref[pair, pl.ds(0, block), :] = s[:block]
        s_ref[pair, pl.ds(block, rows), :] = jnp.where(visible, s[block:], -1e30)
        dp_ref[pair, pl.ds(0, lead), :] = dot(vc[pl.ds(0, lead), :], gt[pair])

    def sums(pair, offset, size, first):
        top = None
        for start in range(0, size, SUB):
            part = jnp.max(s_ref[pair, pl.ds(offset + start, SUB), :].reshape(tile), axis=0)
            top = part if top is None else jnp.maximum(top, part)
        top = jnp.max(top, axis=0, keepdims=True)
        total = jnp.zeros((8, 2 * rows), F32)
        dsum = jnp.zeros((8, 2 * rows), F32)
        for start in range(0, size, SUB):
            here = pl.ds(offset + start, SUB)
            e = jnp.exp2(s_ref[pair, here, :] - top)
            total = total + jnp.sum(e.reshape(tile), axis=0)
            if first:
                dsum = dsum + jnp.sum((e * dp_ref[pair, here, :]).reshape(tile), axis=0)
        if first:
            m_ref[pair] = top
            l_ref[pair] = total
            d_ref[pair] = dsum
        else:
            newest = jnp.maximum(m_ref[pair], top)
            fade, add = jnp.exp2(m_ref[pair] - newest), jnp.exp2(top - newest)
            m_ref[pair] = newest
            l_ref[pair] = l_ref[pair] * fade + total * add
            d_ref[pair] = d_ref[pair] * fade

    def staggered(products, after, unroll, then=None):
        def body(i, carry):
            for j in range(unroll):
                products(i * unroll + j)
                if j:
                    after(i * unroll + j - 1)
            after(i * unroll + unroll - 1)
            if then is not None:
                then(i)
            return carry

        lax.fori_loop(0, pairs // unroll, body, 0)

    def ahead(weights, products, begin, end, step, then=None):
        def body(i, carry):
            first = begin + i * step
            weights(first, 0)
            for j in range(step):
                if j + 1 < step:
                    weights(first + j + 1, (j + 1) % 2)
                products(first + j, j % 2)
            if then is not None:
                then(i)
            return carry

        lax.fori_loop(0, (end - begin) // step, body, 0)

    def key_scores(offset, size):
        def products(pair):
            s_ref[pair, pl.ds(offset, size), :] = dot(kc[pl.ds(offset, size), :], qt[pair])

        staggered(products, lambda pair: sums(pair, offset, size, False), pairs)

    def value_scores(offset, size):
        def products(pair):
            dp_ref[pair, pl.ds(offset, size), :] = dot(vc[pl.ds(offset, size), :], gt[pair])

        def after(pair):
            dsum = d_ref[pair]
            for start in range(0, size, SUB):
                here = pl.ds(offset + start, SUB)
                dsum = dsum + jnp.sum((s_ref[pair, here, :] * dp_ref[pair, here, :]).reshape(tile), axis=0)
            d_ref[pair] = dsum

        staggered(products, after, pairs)

    def value_grads(offset, size, then):
        keys = pl.ds(offset, size)
        dv_acc[keys, :] = jnp.zeros((size, D), F32)
        some = pl.ds(0, size)

        def weights(pair, slot):
            shift = m_ref[pair]
            for start in range(0, size, SUB):
                here = pl.ds(offset + start, SUB)
                p = jnp.exp2(s_ref[pair, here, :] - shift[0:1])
                s_ref[pair, here, :] = p
                to = pl.ds(start, SUB)
                hi, lo = split(p)
                pcat[slot, to, 0 : 2 * rows] = hi
                pcat[slot, to, 2 * rows :] = lo

        def products(pair, slot):
            dv = dot(pcat[slot, some, :], gr[pair])
            dv_acc[keys, :] += dv[:, :D] + dv[:, D:]

        ahead(weights, products, 0, pairs, STEP, then)

    def key_grads(offset, size, first, begin, end):
        keys = pl.ds(offset, size)
        if begin == 0:
            dk_acc[keys, :] = jnp.zeros((size, D), F32)
        some = pl.ds(0, size)

        def weights(pair, slot):
            mean = d_ref[pair][0:1]
            for start in range(0, size, SUB):
                here = pl.ds(offset + start, SUB)
                to = pl.ds(start, SUB)
                hi, lo = split(s_ref[pair, here, :] * (dp_ref[pair, here, :] - mean))
                dcat[slot, to, 0 : 2 * rows] = hi
                dcat[slot, to, 2 * rows :] = lo

        def products(pair, slot):
            dk = dot(dcat[slot, some, :], qr[pair])
            dk_acc[keys, :] += dk[:, :D] + dk[:, D:]
            high = dot(kt[:, keys], dcat[slot, some, 0 : 2 * rows])
            dq = high[:D] + high[D:] + dot(kt[0:D, keys], dcat[slot, some, 2 * rows :])
            if first:
                dqt[pair] = dq
            else:
                dqt[pair] += dq

        ahead(weights, products, begin, end, STEP)

    def lead_grads(begin, end, then):
        size = lead
        keys = some = pl.ds(0, size)
        if begin == 0:
            dk_acc[keys, :] = jnp.zeros((size, D), F32)
            dv_acc[keys, :] = jnp.zeros((size, D), F32)

        def weights(pair, slot):
            shift, mean = m_ref[pair][0:1], d_ref[pair][0:1]
            for start in range(0, size, SUB):
                here = pl.ds(start, SUB)
                p = jnp.exp2(s_ref[pair, here, :] - shift)
                ds = p * (dp_ref[pair, here, :] - mean)
                hi, lo = split(p)
                pcat[slot, here, 0 : 2 * rows] = hi
                pcat[slot, here, 2 * rows :] = lo
                hi, lo = split(ds)
                dcat[slot, here, 0 : 2 * rows] = hi
                dcat[slot, here, 2 * rows :] = lo

        def products(pair, slot):
            dv = dot(pcat[slot, some, :], gr[pair])
            dv_acc[keys, :] += dv[:, :D] + dv[:, D:]
            dk = dot(dcat[slot, some, :], qr[pair])
            dk_acc[keys, :] += dk[:, :D] + dk[:, D:]
            high = dot(kt[:, keys], dcat[slot, some, 0 : 2 * rows])
            dq = high[:D] + high[D:] + dot(kt[0:D, keys], dcat[slot, some, 2 * rows :])
            then(pair, dqt[pair] + dq)

        ahead(weights, products, begin, end, STEP)

    every = range(parts)
    front, last = range(cut), range(cut, parts)
    loops = pairs // STEP

    relay(0, range(1))
    staggered(
        lead_products,
        lambda pair: sums(pair, 0, lead, True),
        STEP,
        lambda i: relay(0, [i + 1]),
    )
    relay(0, range(1 + loops, cut))
    place_keys(kv2.at[0], 0, off2, front_size)
    key_scores(off2, front_size)
    relay(0, range(max(1 + loops, cut), parts))
    place_keys(kv2.at[0], last_at, off2 + last_at, last_size)
    key_scores(off2 + last_at, last_size)
    arrive(0, front)
    place_keys(kv1.at[0], 0, off1, front_size)
    key_scores(off1, front_size)
    relay(1, range(1))
    arrive(0, last)
    place_keys(kv1.at[0], last_at, off1 + last_at, last_size)
    key_scores(off1 + last_at, last_size)
    relay(1, range(1, 2))

    def total(pair, carry):
        l = jnp.sum(l_ref[pair], axis=0, keepdims=True)
        d_ref[pair] = d_ref[pair] / l
        m_ref[pair] = m_ref[pair] + jnp.log2(l)
        return carry

    lax.fori_loop(0, pairs, total, 0)

    acc = (dk_acc, dv_acc)

    def out_y(i, t):
        return remote(
            acc[t].at[pl.ds(off1 + i * SUB, SUB)], ry.at[t, pl.ds(i * SUB, SUB)],
            out_y_send.at[i, t], out_y_recv.at[i, t], (partner, head),
        )

    def out_z(i, t):
        return remote(
            acc[t].at[pl.ds(off2 + i * SUB, SUB)], rz.at[t, pl.ds(i * SUB, SUB)],
            out_z_send.at[i, t], out_z_recv.at[i, t], (above, head),
        )

    def send_y(t, some, when=True):
        @pl.when(when)
        def _():
            for i in some:
                out_y(i, t).start()

    def send_z_odd(t, some):
        @pl.when(odd)
        def _():
            for i in some:
                out_z(i, t).start()

    def join(t, some):
        for i in some:
            out_y(i, t).wait_recv()

            @pl.when(even)
            def _():
                acc[t][pl.ds(off2 + i * SUB, SUB), :] += ry[t, pl.ds(i * SUB, SUB), :]
                out_z(i, t).start()

    width = heads * D
    share = rows // n_head

    def to_peer(step, pair):
        other = lax.rem(head + step, n_head)
        return remote(
            dqs.at[pair, pl.ds(other * share, share), :],
            gq_ref.at[:, pl.ds(pl.multiple_of(head * width + pair * 2 * D, D), 2 * D)],
            q_send.at[step - 1, pair], q_recv.at[step - 1, pair], (seq, other),
        )

    def keep(pair):
        return pltpu.make_async_copy(
            dqs.at[pair, pl.ds(head * share, share), :],
            gq_ref.at[:, pl.ds(pl.multiple_of(head * width + pair * 2 * D, D), 2 * D)],
            q_local.at[pair],
        )

    def stage(pair, dq):
        for half in range(2):
            dqs[pair, :, half * D : (half + 1) * D] = dq[:, half * rows : (half + 1) * rows].T * factor
        for step in range(1, n_head):
            to_peer(step, pair).start()
        keep(pair).start()

    value_grads(off1, block, lambda i: relay(1, [2 + i]))
    send_y(1, every, odd)
    relay(1, range(2 + loops, parts))
    send_y(1, every, even)
    value_grads(off2, block, None)
    send_z_odd(1, every)
    place_values(kv2.at[1], 0, off2, block)
    value_scores(off2, block)
    arrive(1, front)
    place_values(kv1.at[1], 0, off1, front_size)
    value_scores(off1, front_size)
    arrive(1, last)
    place_values(kv1.at[1], last_at, off1 + last_at, last_size)
    value_scores(off1 + last_at, last_size)

    def settle_mean(pair, carry):
        d_ref[pair] = jnp.broadcast_to(jnp.sum(d_ref[pair], axis=0, keepdims=True), (8, 2 * rows))
        return carry

    lax.fori_loop(0, pairs, settle_mean, 0)

    middle = pairs // 2
    key_grads(off1 + last_at, last_size, True, 0, pairs)
    send_y(0, last)
    key_grads(off1, front_size, False, 0, middle)
    key_grads(off2, block, False, 0, middle)
    join(1, every)
    lead_grads(0, middle, stage)
    key_grads(off1, front_size, False, middle, pairs)
    send_y(0, front)
    key_grads(off2, block, False, middle, pairs)
    send_z_odd(0, every)
    join(0, last)
    lead_grads(middle, pairs, stage)
    grk_ref[...] = dk_acc[pl.ds(block, rows), :]
    grv_ref[...] = dv_acc[pl.ds(block, rows), :]
    join(0, front)

    @pl.when(odd)
    def _():
        for t in range(2):
            acc[t][pl.ds(0, block), :] += ry[t]

    out = (gpk_ref, gpv_ref)
    for t in (1, 0):
        for i in (*last, *front):
            here = pl.ds(i * SUB, SUB)
            out_z(i, t).wait_recv()
            out[t][here, :] = acc[t][here, :] + rz[t, here, :]

    for pair in range(pairs):
        keep(pair).wait()
        for step in range(1, n_head):
            to_peer(step, pair).wait()
    for i, t in pieces:
        in_z(i, t).wait_send()
        in_y_own(i, t).wait_send()
        out_y(i, t).wait_send()
        out_z(i, t).wait_send()


def settle(*refs):
    count = (len(refs) - 2) // 3
    load_sem, store_sem = refs[-2:]
    held = refs[2 * count : 3 * count]
    loads = [
        pltpu.make_async_copy(refs[i], held[i], load_sem.at[i]) for i in range(count)
    ]
    stores = [
        pltpu.make_async_copy(held[i], refs[count + i], store_sem.at[i]) for i in range(count)
    ]
    for load in loads:
        load.start()
    for load, store in zip(loads, stores):
        load.wait()
        store.start()
    for store in stores:
        store.wait()


def per_device(n_seq, n_head, queries, prefix_keys, prefix_value_rows, response_keys, response_values, out_grad, lengths):
    rows, width = queries.shape
    block = prefix_keys.shape[0]
    assert prefix_keys.shape[1] == D
    heads = width // D
    pairs = heads // 2
    keys = WINDOW * block + rows
    lead = block + rows
    vmem = pl.BlockSpec(memory_space=pltpu.VMEM)
    anywhere = pl.BlockSpec(memory_space=pl.ANY)
    part_sems = pltpu.SemaphoreType.DMA((block // SUB, 2))
    shape = jax.ShapeDtypeStruct
    results = pl.pallas_call(
        functools.partial(kernel, n_seq, n_head),
        out_shape=(
            shape((rows // n_head, width * n_head), F32),
            shape((block, D), F32),
            shape((block, D), F32),
            shape((rows, D), F32),
            shape((rows, D), F32),
        ),
        in_specs=[pl.BlockSpec(memory_space=pltpu.SMEM)] + [anywhere] * 6,
        out_specs=(pl.BlockSpec(memory_space=pl.ANY), vmem, vmem, vmem, vmem),
        scratch_shapes=[
            pltpu.VMEM((rows, width), F32),
            pltpu.VMEM((rows, width), F32),
            pltpu.VMEM((2, block, D), F32),
            pltpu.VMEM((2, block, D), F32),
            pltpu.VMEM((2, block, D), F32),
            pltpu.VMEM((2, rows, D), F32),
            pltpu.VMEM((keys, 3 * D), BF16),
            pltpu.VMEM((keys, 3 * D), BF16),
            pltpu.VMEM((2 * D, keys), BF16),
            pltpu.VMEM((pairs, 3 * D, 2 * rows), BF16),
            pltpu.VMEM((pairs, 3 * D, 2 * rows), BF16),
            pltpu.VMEM((pairs, 4 * rows, 2 * D), BF16),
            pltpu.VMEM((pairs, 4 * rows, 2 * D), BF16),
            pltpu.VMEM((pairs, keys, 2 * rows), F32),
            pltpu.VMEM((pairs, keys, 2 * rows), F32),
            pltpu.VMEM((pairs, 1, 2 * rows), F32),
            pltpu.VMEM((pairs, 8, 2 * rows), F32),
            pltpu.VMEM((pairs, 8, 2 * rows), F32),
            pltpu.VMEM((2, lead, 4 * rows), BF16),
            pltpu.VMEM((2, lead, 4 * rows), BF16),
            pltpu.VMEM((keys, D), F32),
            pltpu.VMEM((keys, D), F32),
            pltpu.VMEM((pairs, D, 2 * rows), F32),
            pltpu.VMEM((pairs, rows, 2 * D), F32),
            pltpu.VMEM((2, block, D), F32),
            pltpu.VMEM((2, block, D), F32),
        ]
        + [part_sems] * 8
        + [pltpu.SemaphoreType.DMA((n_head - 1, pairs))] * 2
        + [pltpu.SemaphoreType.DMA((pairs,)), pltpu.SemaphoreType.DMA((6,))],
        compiler_params=pltpu.CompilerParams(
            collective_id=0, has_side_effects=True, vmem_limit_bytes=63 * 1024 * 1024
        ),
    )(lengths, queries, prefix_keys, prefix_value_rows, response_keys, response_values, out_grad)
    return pl.pallas_call(
        settle,
        out_shape=tuple(shape(x.shape, x.dtype) for x in results),
        in_specs=[anywhere] * len(results),
        out_specs=(anywhere,) * len(results),
        scratch_shapes=[pltpu.VMEM(x.shape, x.dtype) for x in results]
        + [pltpu.SemaphoreType.DMA((len(results),))] * 2,
    )(*results)


def solution(mesh):
    sharded = P("seq", "head")
    return jax.shard_map(
        functools.partial(per_device, mesh.shape["seq"], mesh.shape["head"]),
        mesh=mesh,
        in_specs=(sharded,) * 6 + (P("seq"),),
        out_specs=(P(("seq", "head"), None),) + (sharded,) * 4,
        check_vma=False,
    )
```

```python
import functools
import math

import jax
import jax.numpy as jnp
from jax import lax
from jax.experimental import pallas as pl
from jax.experimental.pallas import tpu as pltpu
from jax.sharding import PartitionSpec as P

HEAD_SIZE = 128
WINDOW = 3
D = HEAD_SIZE
MESH = pl.DeviceIdType.MESH
F32, BF16 = jnp.float32, jnp.bfloat16
SUB = 128
STEP = 4


def split(x):
    hi = x.astype(BF16)
    lo = (x - hi.astype(F32)).astype(BF16)
    return hi, lo


def dot(a, b):
    return jnp.dot(a, b, preferred_element_type=F32)


def kernel(
    n_seq, n_head,
    length_ref, q_hbm, pk_ref, pv_ref, rk_ref, rv_ref, g_hbm,
    gq_ref, gpk_ref, gpv_ref, grk_ref, grv_ref,
    q_ref, g_ref, kv0, kv1, kv2, kvr, kc, vc, kt, qt, gt, qr, gr, s_ref, dp_ref, m_ref, l_ref, d_ref,
    pcat, dcat, dk_acc, dv_acc, dqt, dqs, ry, rz,
    in_z_send, in_z_recv, in_y_send, in_y_recv,
    out_z_send, out_z_recv, out_y_send, out_y_recv,
    q_send, q_recv, q_local, load_sem,
):
    rows = q_hbm.shape[0]
    heads = q_hbm.shape[1] // D
    pairs = heads // 2
    block = pk_ref.shape[0]
    parts = block // SUB
    lead = block + rows
    cut = (parts + 1) // 2
    front_size, last_at, last_size = cut * SUB, cut * SUB, block - cut * SUB
    off1, off2 = lead, lead + block
    factor = D ** (-0.5)
    seq = lax.axis_index("seq")
    head = lax.axis_index("head")
    even = lax.rem(seq, 2) == 0
    odd = jnp.logical_not(even)
    partner = seq + 1 - 2 * lax.rem(seq, 2)
    below = lax.rem(seq + n_seq - 2, n_seq)
    above = lax.rem(seq + 2, n_seq)

    barrier = pltpu.get_barrier_semaphore()
    for other in (partner, below, above):
        pl.semaphore_signal(barrier, inc=1, device_id=(other, head), device_id_type=MESH)
    for step in range(1, n_head):
        pl.semaphore_signal(
            barrier, inc=1, device_id=(seq, lax.rem(head + step, n_head)), device_id_type=MESH
        )
    loads = [
        pltpu.make_async_copy(src, dst, load_sem.at[i])
        for i, (src, dst) in enumerate(
            (
                (pk_ref, kv0.at[0]),
                (pv_ref, kv0.at[1]),
                (rk_ref, kvr.at[0]),
                (rv_ref, kvr.at[1]),
                (q_hbm, q_ref),
                (g_hbm, g_ref),
            )
        )
    ]
    for load in loads:
        load.start()
    pl.semaphore_wait(barrier, 3 + n_head - 1)

    def remote(src, dst, send, recv, to):
        return pltpu.make_async_remote_copy(
            src_ref=src, dst_ref=dst, send_sem=send, recv_sem=recv,
            device_id=to, device_id_type=MESH,
        )

    own = (kv0.at[0], kv0.at[1])

    def piece(i):
        return pl.ds(i * SUB, SUB)

    def in_z(i, t):
        return remote(own[t].at[piece(i)], kv2.at[t, piece(i)], in_z_send.at[i, t], in_z_recv.at[i, t], (below, head))

    def in_y_own(i, t):
        return remote(own[t].at[piece(i)], kv1.at[t, piece(i)], in_y_send.at[i, t], in_y_recv.at[i, t], (partner, head))

    def in_y_pass(i, t):
        return remote(kv2.at[t, piece(i)], kv1.at[t, piece(i)], in_y_send.at[i, t], in_y_recv.at[i, t], (partner, head))

    pieces = [(i, t) for t in range(2) for i in range(parts)]
    for load in loads[:2]:
        load.wait()
    for i, t in pieces:
        in_z(i, t).start()

    @pl.when(odd)
    def _():
        for i, t in pieces:
            in_y_own(i, t).start()

    def relay(t, some):
        for i in some:
            in_z(i, t).wait_recv()

            @pl.when(even)
            def _():
                in_y_pass(i, t).start()

    def arrive(t, some):
        for i in some:
            in_y_own(i, t).wait_recv()

    def place_keys(keys, first, offset, size):
        for start in range(0, size, SUB):
            here = pl.ds(offset + start, SUB)
            k = keys[pl.ds(first + start, SUB), :]
            hi, lo = split(k)
            kc[here, 0:D] = hi
            kc[here, D : 2 * D] = lo
            kc[here, 2 * D : 3 * D] = hi
            hi, lo = split(k.T)
            kt[0:D, here] = hi
            kt[D : 2 * D, here] = lo

    def place_values(values, first, offset, size):
        for start in range(0, size, SUB):
            here = pl.ds(offset + start, SUB)
            hi, lo = split(values[pl.ds(first + start, SUB), :])
            vc[here, 0:D] = hi
            vc[here, D : 2 * D] = lo
            vc[here, 2 * D : 3 * D] = hi

    for load in loads[2:4]:
        load.wait()
    place_keys(kv0.at[0], 0, 0, block)
    place_values(kv0.at[1], 0, 0, block)
    place_keys(kvr.at[0], 0, block, rows)
    place_values(kvr.at[1], 0, block, rows)
    for load in loads[4:]:
        load.wait()

    length = length_ref[0]
    token = lax.broadcasted_iota(jnp.int32, (rows, 1), 0)
    live = token < length
    for h in range(heads):
        cols = pl.ds(h * D, D)
        pair, half = h // 2, h % 2
        lanes = pl.ds(half * rows, rows)
        q = q_ref[:, cols]
        g = jnp.where(live, g_ref[:, cols], 0.0)
        for x, wide, tall, scale in (
            (q, qr, qt, factor * math.log2(math.e)),
            (g, gr, gt, 1.0),
        ):
            hi, lo = split((x * scale).T)
            tall[pair, 0:D, lanes] = hi
            tall[pair, D : 2 * D, lanes] = hi
            tall[pair, 2 * D : 3 * D, lanes] = lo
            hi, lo = split(x * factor) if wide is qr else split(x)
            for copy in range(2):
                at_rows = pl.ds(copy * 2 * rows + half * rows, rows)
                wide[pair, at_rows, 0:D] = hi
                wide[pair, at_rows, D : 2 * D] = lo

    tile = (SUB // 8, 8, 2 * rows)

    def lead_products(pair):
        s = dot(kc[pl.ds(0, lead), :], qt[pair])
        slot = lax.broadcasted_iota(jnp.int32, (rows, 2 * rows), 0)
        lane = lax.broadcasted_iota(jnp.int32, (rows, 2 * rows), 1)
        query = jnp.where(lane >= rows, lane - rows, lane)
        visible = (slot <= query) & (slot < length)
        s_ref[pair, pl.ds(0, block), :] = s[:block]
        s_ref[pair, pl.ds(block, rows), :] = jnp.where(visible, s[block:], -1e30)
        dp_ref[pair, pl.ds(0, lead), :] = dot(vc[pl.ds(0, lead), :], gt[pair])

    def sums(pair, offset, size, first):
        top = None
        for start in range(0, size, SUB):
            part = jnp.max(s_ref[pair, pl.ds(offset + start, SUB), :].reshape(tile), axis=0)
            top = part if top is None else jnp.maximum(top, part)
        top = jnp.max(top, axis=0, keepdims=True)
        total = jnp.zeros((8, 2 * rows), F32)
        dsum = jnp.zeros((8, 2 * rows), F32)
        for start in range(0, size, SUB):
            here = pl.ds(offset + start, SUB)
            e = jnp.exp2(s_ref[pair, here, :] - top)
            total = total + jnp.sum(e.reshape(tile), axis=0)
            if first:
                dsum = dsum + jnp.sum((e * dp_ref[pair, here, :]).reshape(tile), axis=0)
        if first:
            m_ref[pair] = top
            l_ref[pair] = total
            d_ref[pair] = dsum
        else:
            newest = jnp.maximum(m_ref[pair], top)
            fade, add = jnp.exp2(m_ref[pair] - newest), jnp.exp2(top - newest)
            m_ref[pair] = newest
            l_ref[pair] = l_ref[pair] * fade + total * add
            d_ref[pair] = d_ref[pair] * fade

    def staggered(products, after, unroll, then=None):
        def body(i, carry):
            for j in range(unroll):
                products(i * unroll + j)
                if j:
                    after(i * unroll + j - 1)
            after(i * unroll + unroll - 1)
            if then is not None:
                then(i)
            return carry

        lax.fori_loop(0, pairs // unroll, body, 0)

    def ahead(weights, products, begin, end, step, then=None):
        def body(i, carry):
            first = begin + i * step
            weights(first, 0)
            for j in range(step):
                if j + 1 < step:
                    weights(first + j + 1, (j + 1) % 2)
                products(first + j, j % 2)
            if then is not None:
                then(i)
            return carry

        lax.fori_loop(0, (end - begin) // step, body, 0)

    def key_scores(offset, size):
        def products(pair):
            s_ref[pair, pl.ds(offset, size), :] = dot(kc[pl.ds(offset, size), :], qt[pair])

        staggered(products, lambda pair: sums(pair, offset, size, False), pairs)

    def value_scores(offset, size):
        def products(pair):
            dp_ref[pair, pl.ds(offset, size), :] = dot(vc[pl.ds(offset, size), :], gt[pair])

        def after(pair):
            dsum = d_ref[pair]
            for start in range(0, size, SUB):
                here = pl.ds(offset + start, SUB)
                dsum = dsum + jnp.sum((s_ref[pair, here, :] * dp_ref[pair, here, :]).reshape(tile), axis=0)
            d_ref[pair] = dsum

        staggered(products, after, pairs)

    def value_grads(offset, size, then):
        keys = pl.ds(offset, size)
        dv_acc[keys, :] = jnp.zeros((size, D), F32)
        some = pl.ds(0, size)

        def weights(pair, slot):
            shift = m_ref[pair]
            for start in range(0, size, SUB):
                here = pl.ds(offset + start, SUB)
                p = jnp.exp2(s_ref[pair, here, :] - shift[0:1])
                s_ref[pair, here, :] = p
                to = pl.ds(start, SUB)
                hi, lo = split(p)
                pcat[slot, to, 0 : 2 * rows] = hi
                pcat[slot, to, 2 * rows :] = lo

        def products(pair, slot):
            dv = dot(pcat[slot, some, :], gr[pair])
            dv_acc[keys, :] += dv[:, :D] + dv[:, D:]

        ahead(weights, products, 0, pairs, STEP, then)

    def key_grads(offset, size, first, begin, end):
        keys = pl.ds(offset, size)
        if begin == 0:
            dk_acc[keys, :] = jnp.zeros((size, D), F32)
        some = pl.ds(0, size)

        def weights(pair, slot):
            mean = d_ref[pair][0:1]
            for start in range(0, size, SUB):
                here = pl.ds(offset + start, SUB)
                to = pl.ds(start, SUB)
                hi, lo = split(s_ref[pair, here, :] * (dp_ref[pair, here, :] - mean))
                dcat[slot, to, 0 : 2 * rows] = hi
                dcat[slot, to, 2 * rows :] = lo

        def products(pair, slot):
            dk = dot(dcat[slot, some, :], qr[pair])
            dk_acc[keys, :] += dk[:, :D] + dk[:, D:]
            high = dot(kt[:, keys], dcat[slot, some, 0 : 2 * rows])
            dq = high[:D] + high[D:] + dot(kt[0:D, keys], dcat[slot, some, 2 * rows :])
            if first:
                dqt[pair] = dq
            else:
                dqt[pair] += dq

        ahead(weights, products, begin, end, STEP if (end - begin) % STEP == 0 else 2)

    def lead_queries(begin, end, then):
        keys = pl.ds(0, lead)

        def weights(pair, slot):
            shift, mean = m_ref[pair], d_ref[pair][0:1]
            for start in range(0, lead, SUB):
                here = pl.ds(start, SUB)
                p = jnp.exp2(s_ref[pair, here, :] - shift)
                ds = p * (dp_ref[pair, here, :] - mean)
                s_ref[pair, here, :] = p
                dp_ref[pair, here, :] = ds
                hi, lo = split(ds)
                dcat[slot, here, 0 : 2 * rows] = hi
                dcat[slot, here, 2 * rows :] = lo

        def products(pair, slot):
            high = dot(kt[:, keys], dcat[slot, :, 0 : 2 * rows])
            dq = high[:D] + high[D:] + dot(kt[0:D, keys], dcat[slot, :, 2 * rows :])
            then(pair, dqt[pair] + dq)

        ahead(weights, products, begin, end, 2)

    def lead_grads(then):
        dk_acc[pl.ds(0, lead), :] = jnp.zeros((lead, D), F32)
        dv_acc[pl.ds(0, lead), :] = jnp.zeros((lead, D), F32)

        def weights(pair, slot):
            for start in range(0, lead, SUB):
                here = pl.ds(start, SUB)
                hi, lo = split(s_ref[pair, here, :])
                pcat[slot, here, 0 : 2 * rows] = hi
                pcat[slot, here, 2 * rows :] = lo
                hi, lo = split(dp_ref[pair, here, :])
                dcat[slot, here, 0 : 2 * rows] = hi
                dcat[slot, here, 2 * rows :] = lo

        def products(pair, slot):
            dv = dot(pcat[slot], gr[pair])
            dv_acc[pl.ds(0, lead), :] += dv[:, :D] + dv[:, D:]
            dk = dot(dcat[slot], qr[pair])
            dk_acc[pl.ds(0, lead), :] += dk[:, :D] + dk[:, D:]

        ahead(weights, products, 0, pairs, 2, then)

    every, front, last = range(parts), range(cut), range(cut, parts)
    loops = pairs // STEP
    assert cut - 1 <= pairs // 2 and parts > 1 + loops

    relay(0, range(1))
    staggered(
        lead_products,
        lambda pair: sums(pair, 0, lead, True),
        STEP,
        lambda i: relay(0, [i + 1]),
    )
    relay(0, range(1 + loops, cut))
    place_keys(kv2.at[0], 0, off2, front_size)
    key_scores(off2, front_size)
    relay(0, range(max(1 + loops, cut), parts))
    place_keys(kv2.at[0], last_at, off2 + last_at, last_size)
    key_scores(off2 + last_at, last_size)
    arrive(0, front)
    place_keys(kv1.at[0], 0, off1, front_size)
    key_scores(off1, front_size)
    relay(1, range(1))
    arrive(0, last)
    place_keys(kv1.at[0], last_at, off1 + last_at, last_size)
    key_scores(off1 + last_at, last_size)
    relay(1, range(1, 2))

    def total(pair, carry):
        l = jnp.sum(l_ref[pair], axis=0, keepdims=True)
        d_ref[pair] = d_ref[pair] / l
        m_ref[pair] = m_ref[pair] + jnp.log2(l)
        return carry

    lax.fori_loop(0, pairs, total, 0)

    acc = (dk_acc, dv_acc)

    def out_y(i, t):
        return remote(
            acc[t].at[pl.ds(off1 + i * SUB, SUB)], ry.at[t, pl.ds(i * SUB, SUB)],
            out_y_send.at[i, t], out_y_recv.at[i, t], (partner, head),
        )

    def out_z(i, t):
        return remote(
            acc[t].at[pl.ds(off2 + i * SUB, SUB)], rz.at[t, pl.ds(i * SUB, SUB)],
            out_z_send.at[i, t], out_z_recv.at[i, t], (above, head),
        )

    def send_y(t, some, when=True):
        @pl.when(when)
        def _():
            for i in some:
                out_y(i, t).start()

    def send_z_odd(t, some):
        @pl.when(odd)
        def _():
            for i in some:
                out_z(i, t).start()

    def join(t, some):
        for i in some:
            out_y(i, t).wait_recv()

            @pl.when(even)
            def _():
                acc[t][pl.ds(off2 + i * SUB, SUB), :] += ry[t, pl.ds(i * SUB, SUB), :]
                out_z(i, t).start()

    width = heads * D
    share = rows // n_head

    def to_peer(step, pair):
        other = lax.rem(head + step, n_head)
        return remote(
            dqs.at[pair, pl.ds(other * share, share), :],
            gq_ref.at[:, pl.ds(pl.multiple_of(head * width + pair * 2 * D, D), 2 * D)],
            q_send.at[step - 1, pair], q_recv.at[step - 1, pair], (seq, other),
        )

    def keep(pair):
        return pltpu.make_async_copy(
            dqs.at[pair, pl.ds(head * share, share), :],
            gq_ref.at[:, pl.ds(pl.multiple_of(head * width + pair * 2 * D, D), 2 * D)],
            q_local.at[pair],
        )

    def stage(pair, dq):
        for half in range(2):
            dqs[pair, :, half * D : (half + 1) * D] = dq[:, half * rows : (half + 1) * rows].T * factor
        for step in range(1, n_head):
            to_peer(step, pair).start()
        keep(pair).start()

    value_grads(off1, block, lambda i: relay(1, [2 + i]))
    send_y(1, every, odd)
    relay(1, range(2 + loops, parts))
    send_y(1, every, even)
    value_grads(off2, block, None)
    send_z_odd(1, every)
    place_values(kv2.at[1], 0, off2, block)
    value_scores(off2, block)
    arrive(1, front)
    place_values(kv1.at[1], 0, off1, front_size)
    value_scores(off1, front_size)
    join(1, range(1))
    arrive(1, last)
    place_values(kv1.at[1], last_at, off1 + last_at, last_size)
    value_scores(off1 + last_at, last_size)

    def settle_mean(pair, carry):
        d_ref[pair] = jnp.broadcast_to(jnp.sum(d_ref[pair], axis=0, keepdims=True), (8, 2 * rows))
        return carry

    lax.fori_loop(0, pairs, settle_mean, 0)

    quarter = pairs // 4
    key_grads(off1 + last_at, last_size, True, 0, pairs)
    send_y(0, last)
    join(1, range(1, 3))
    key_grads(off1, front_size, False, 0, pairs)
    send_y(0, front)
    join(1, range(3, parts))
    key_grads(off2, block, False, 0, quarter)
    lead_queries(0, quarter, stage)
    key_grads(off2, block, False, quarter, pairs)
    send_z_odd(0, every)
    join(0, last)
    lead_queries(quarter, pairs, stage)
    join(0, range(1))

    def join_front(i):
        @pl.when(i < cut - 1)
        def _():
            join(0, [i + 1])

    lead_grads(join_front)
    grk_ref[...] = dk_acc[pl.ds(block, rows), :]
    grv_ref[...] = dv_acc[pl.ds(block, rows), :]

    @pl.when(odd)
    def _():
        for t in range(2):
            acc[t][pl.ds(0, block), :] += ry[t]

    out = (gpk_ref, gpv_ref)
    for t in (1, 0):
        for i in every:
            here = pl.ds(i * SUB, SUB)
            out_z(i, t).wait_recv()
            out[t][here, :] = acc[t][here, :] + rz[t, here, :]

    for pair in range(pairs):
        keep(pair).wait()
        for step in range(1, n_head):
            to_peer(step, pair).wait()
    for i, t in pieces:
        in_z(i, t).wait_send()
        in_y_own(i, t).wait_send()
        out_y(i, t).wait_send()
        out_z(i, t).wait_send()


def settle(*refs):
    count = (len(refs) - 1) // 2
    store_sem = refs[-1]
    stores = [
        pltpu.make_async_copy(refs[i], refs[count + i], store_sem.at[i]) for i in range(count)
    ]
    for store in stores:
        store.start()
    for store in stores:
        store.wait()


def per_device(n_seq, n_head, queries, prefix_keys, prefix_value_rows, response_keys, response_values, out_grad, lengths):
    rows, width = queries.shape
    block = prefix_keys.shape[0]
    assert prefix_keys.shape[1] == D
    heads = width // D
    pairs = heads // 2
    keys = WINDOW * block + rows
    lead = block + rows
    vmem = pl.BlockSpec(memory_space=pltpu.VMEM)
    anywhere = pl.BlockSpec(memory_space=pl.ANY)
    part_sems = pltpu.SemaphoreType.DMA((block // SUB, 2))
    shape = jax.ShapeDtypeStruct
    results = pl.pallas_call(
        functools.partial(kernel, n_seq, n_head),
        out_shape=(
            pltpu.VMEM((rows // n_head, width * n_head), F32),
            pltpu.VMEM((block, D), F32),
            pltpu.VMEM((block, D), F32),
            pltpu.VMEM((rows, D), F32),
            pltpu.VMEM((rows, D), F32),
        ),
        in_specs=[pl.BlockSpec(memory_space=pltpu.SMEM)] + [anywhere] * 6,
        out_specs=(vmem,) * 5,
        scratch_shapes=[
            pltpu.VMEM((rows, width), F32),
            pltpu.VMEM((rows, width), F32),
            pltpu.VMEM((2, block, D), F32),
            pltpu.VMEM((2, block, D), F32),
            pltpu.VMEM((2, block, D), F32),
            pltpu.VMEM((2, rows, D), F32),
            pltpu.VMEM((keys, 3 * D), BF16),
            pltpu.VMEM((keys, 3 * D), BF16),
            pltpu.VMEM((2 * D, keys), BF16),
            pltpu.VMEM((pairs, 3 * D, 2 * rows), BF16),
            pltpu.VMEM((pairs, 3 * D, 2 * rows), BF16),
            pltpu.VMEM((pairs, 4 * rows, 2 * D), BF16),
            pltpu.VMEM((pairs, 4 * rows, 2 * D), BF16),
            pltpu.VMEM((pairs, keys, 2 * rows), F32),
            pltpu.VMEM((pairs, keys, 2 * rows), F32),
            pltpu.VMEM((pairs, 1, 2 * rows), F32),
            pltpu.VMEM((pairs, 8, 2 * rows), F32),
            pltpu.VMEM((pairs, 8, 2 * rows), F32),
            pltpu.VMEM((2, lead, 4 * rows), BF16),
            pltpu.VMEM((2, lead, 4 * rows), BF16),
            pltpu.VMEM((keys, D), F32),
            pltpu.VMEM((keys, D), F32),
            pltpu.VMEM((pairs, D, 2 * rows), F32),
            pltpu.VMEM((pairs, rows, 2 * D), F32),
            pltpu.VMEM((2, block, D), F32),
            pltpu.VMEM((2, block, D), F32),
        ]
        + [part_sems] * 8
        + [pltpu.SemaphoreType.DMA((n_head - 1, pairs))] * 2
        + [pltpu.SemaphoreType.DMA((pairs,)), pltpu.SemaphoreType.DMA((6,))],
        compiler_params=pltpu.CompilerParams(
            collective_id=0, has_side_effects=True, vmem_limit_bytes=65000000
        ),
    )(lengths, queries, prefix_keys, prefix_value_rows, response_keys, response_values, out_grad)
    return pl.pallas_call(
        settle,
        out_shape=tuple(shape(x.shape, x.dtype) for x in results),
        in_specs=[vmem] * len(results),
        out_specs=(anywhere,) * len(results),
        scratch_shapes=[pltpu.SemaphoreType.DMA((len(results),))],
        compiler_params=pltpu.CompilerParams(vmem_limit_bytes=8 * 1024 * 1024),
    )(*(pltpu.with_memory_space_constraint(x, pltpu.VMEM) for x in results))


def solution(mesh):
    sharded = P("seq", "head")
    return jax.shard_map(
        functools.partial(per_device, mesh.shape["seq"], mesh.shape["head"]),
        mesh=mesh,
        in_specs=(sharded,) * 6 + (P("seq"),),
        out_specs=(P(("seq", "head"), None),) + (sharded,) * 4,
        check_vma=False,
    )
```

```python
import functools
import math

import jax
import jax.numpy as jnp
from jax import lax
from jax.experimental import pallas as pl
from jax.experimental.pallas import tpu as pltpu
from jax.sharding import PartitionSpec as P

HEAD_SIZE = 128
WINDOW = 3
D = HEAD_SIZE
MESH = pl.DeviceIdType.MESH
F32, BF16 = jnp.float32, jnp.bfloat16
SUB = 128
STEP = 4


def split(x):
    hi = x.astype(BF16)
    lo = (x - hi.astype(F32)).astype(BF16)
    return hi, lo


def dot(a, b):
    return jnp.dot(a, b, preferred_element_type=F32)


def kernel(
    n_seq, n_head,
    length_ref, q_hbm, pk_ref, pv_ref, rk_ref, rv_ref, g_hbm,
    gq_ref, gpk_ref, gpv_ref, grk_ref, grv_ref,
    q_ref, g_ref, kv0, kv1, kv2, kvr, kc, vc, kt, qt, gt, qr, gr, s_ref, dp_ref, m_ref, l_ref, d_ref,
    pcat, dcat, dk_acc, dv_acc, dqt, dqs, ry, rz,
    in_z_send, in_z_recv, in_y_send, in_y_recv,
    out_z_send, out_z_recv, out_y_send, out_y_recv,
    q_send, q_recv, q_local, load_sem,
):
    rows = q_hbm.shape[0]
    heads = q_hbm.shape[1] // D
    pairs = heads // 2
    block = pk_ref.shape[0]
    parts = block // SUB
    lead = block + rows
    cut = (parts + 1) // 2
    front_size, last_at, last_size = cut * SUB, cut * SUB, block - cut * SUB
    off1, off2 = lead, lead + block
    factor = D ** (-0.5)
    seq = lax.axis_index("seq")
    head = lax.axis_index("head")
    even = lax.rem(seq, 2) == 0
    odd = jnp.logical_not(even)
    partner = seq + 1 - 2 * lax.rem(seq, 2)
    below = lax.rem(seq + n_seq - 2, n_seq)
    above = lax.rem(seq + 2, n_seq)

    barrier = pltpu.get_barrier_semaphore()
    for other in (partner, below, above):
        pl.semaphore_signal(barrier, inc=1, device_id=(other, head), device_id_type=MESH)
    for step in range(1, n_head):
        pl.semaphore_signal(
            barrier, inc=1, device_id=(seq, lax.rem(head + step, n_head)), device_id_type=MESH
        )
    loads = [
        pltpu.make_async_copy(src, dst, load_sem.at[i])
        for i, (src, dst) in enumerate(
            (
                (pk_ref, kv0.at[0]),
                (pv_ref, kv0.at[1]),
                (rk_ref, kvr.at[0]),
                (rv_ref, kvr.at[1]),
                (q_hbm, q_ref),
                (g_hbm, g_ref),
            )
        )
    ]
    for load in loads:
        load.start()
    pl.semaphore_wait(barrier, 3 + n_head - 1)

    def remote(src, dst, send, recv, to):
        return pltpu.make_async_remote_copy(
            src_ref=src, dst_ref=dst, send_sem=send, recv_sem=recv,
            device_id=to, device_id_type=MESH,
        )

    own = (kv0.at[0], kv0.at[1])

    def piece(i):
        return pl.ds(i * SUB, SUB)

    def in_z(i, t):
        return remote(own[t].at[piece(i)], kv2.at[t, piece(i)], in_z_send.at[i, t], in_z_recv.at[i, t], (below, head))

    def in_y_own(i, t):
        return remote(own[t].at[piece(i)], kv1.at[t, piece(i)], in_y_send.at[i, t], in_y_recv.at[i, t], (partner, head))

    def in_y_pass(i, t):
        return remote(kv2.at[t, piece(i)], kv1.at[t, piece(i)], in_y_send.at[i, t], in_y_recv.at[i, t], (partner, head))

    pieces = [(i, t) for t in range(2) for i in range(parts)]
    for load in loads[:2]:
        load.wait()
    for i, t in pieces:
        in_z(i, t).start()

    @pl.when(odd)
    def _():
        for i, t in pieces:
            in_y_own(i, t).start()

    def relay(t, some):
        for i in some:
            in_z(i, t).wait_recv()

            @pl.when(even)
            def _():
                in_y_pass(i, t).start()

    def arrive(t, some):
        for i in some:
            in_y_own(i, t).wait_recv()

    def place_keys(keys, first, offset, size):
        for start in range(0, size, SUB):
            here = pl.ds(offset + start, SUB)
            k = keys[pl.ds(first + start, SUB), :]
            hi, lo = split(k)
            kc[here, 0:D] = hi
            kc[here, D : 2 * D] = lo
            kc[here, 2 * D : 3 * D] = hi
            hi, lo = split(k.T)
            kt[0:D, here] = hi
            kt[D : 2 * D, here] = lo

    def place_values(values, first, offset, size):
        for start in range(0, size, SUB):
            here = pl.ds(offset + start, SUB)
            hi, lo = split(values[pl.ds(first + start, SUB), :])
            vc[here, 0:D] = hi
            vc[here, D : 2 * D] = lo
            vc[here, 2 * D : 3 * D] = hi

    for load in loads[2:4]:
        load.wait()
    place_keys(kv0.at[0], 0, 0, block)
    place_values(kv0.at[1], 0, 0, block)
    place_keys(kvr.at[0], 0, block, rows)
    place_values(kvr.at[1], 0, block, rows)
    for load in loads[4:]:
        load.wait()

    length = length_ref[0]
    token = lax.broadcasted_iota(jnp.int32, (rows, 1), 0)
    live = token < length
    for h in range(heads):
        cols = pl.ds(h * D, D)
        pair, half = h // 2, h % 2
        lanes = pl.ds(half * rows, rows)
        q = q_ref[:, cols]
        g = jnp.where(live, g_ref[:, cols], 0.0)
        for x, wide, tall, scale in (
            (q, qr, qt, factor * math.log2(math.e)),
            (g, gr, gt, 1.0),
        ):
            hi, lo = split((x * scale).T)
            tall[pair, 0:D, lanes] = hi
            tall[pair, D : 2 * D, lanes] = hi
            tall[pair, 2 * D : 3 * D, lanes] = lo
            hi, lo = split(x * factor) if wide is qr else split(x)
            for copy in range(2):
                at_rows = pl.ds(copy * 2 * rows + half * rows, rows)
                wide[pair, at_rows, 0:D] = hi
                wide[pair, at_rows, D : 2 * D] = lo

    tile = (SUB // 8, 8, 2 * rows)

    def lead_products(pair):
        s = dot(kc[pl.ds(0, lead), :], qt[pair])
        slot = lax.broadcasted_iota(jnp.int32, (rows, 2 * rows), 0)
        lane = lax.broadcasted_iota(jnp.int32, (rows, 2 * rows), 1)
        query = jnp.where(lane >= rows, lane - rows, lane)
        visible = (slot <= query) & (slot < length)
        s_ref[pair, pl.ds(0, block), :] = s[:block]
        s_ref[pair, pl.ds(block, rows), :] = jnp.where(visible, s[block:], -1e30)
        dp_ref[pair, pl.ds(0, lead), :] = dot(vc[pl.ds(0, lead), :], gt[pair])

    def sums(pair, offset, size, first):
        top = None
        for start in range(0, size, SUB):
            part = jnp.max(s_ref[pair, pl.ds(offset + start, SUB), :].reshape(tile), axis=0)
            top = part if top is None else jnp.maximum(top, part)
        top = jnp.max(top, axis=0, keepdims=True)
        total = jnp.zeros((8, 2 * rows), F32)
        dsum = jnp.zeros((8, 2 * rows), F32)
        for start in range(0, size, SUB):
            here = pl.ds(offset + start, SUB)
            e = jnp.exp2(s_ref[pair, here, :] - top)
            total = total + jnp.sum(e.reshape(tile), axis=0)
            if first:
                dsum = dsum + jnp.sum((e * dp_ref[pair, here, :]).reshape(tile), axis=0)
        if first:
            m_ref[pair] = top
            l_ref[pair] = total
            d_ref[pair] = dsum
        else:
            newest = jnp.maximum(m_ref[pair], top)
            fade, add = jnp.exp2(m_ref[pair] - newest), jnp.exp2(top - newest)
            m_ref[pair] = newest
            l_ref[pair] = l_ref[pair] * fade + total * add
            d_ref[pair] = d_ref[pair] * fade

    def staggered(products, after, unroll, then=None):
        def body(i, carry):
            for j in range(unroll):
                products(i * unroll + j)
                if j:
                    after(i * unroll + j - 1)
            after(i * unroll + unroll - 1)
            if then is not None:
                then(i)
            return carry

        lax.fori_loop(0, pairs // unroll, body, 0)

    def ahead(weights, products, begin, end, step, then=None):
        def body(i, carry):
            first = begin + i * step
            weights(first, 0)
            for j in range(step):
                if j + 1 < step:
                    weights(first + j + 1, (j + 1) % 2)
                products(first + j, j % 2)
            if then is not None:
                then(i)
            return carry

        lax.fori_loop(0, (end - begin) // step, body, 0)

    def key_scores(offset, size):
        def products(pair):
            s_ref[pair, pl.ds(offset, size), :] = dot(kc[pl.ds(offset, size), :], qt[pair])

        staggered(products, lambda pair: sums(pair, offset, size, False), pairs)

    def value_scores(offset, size):
        def products(pair):
            dp_ref[pair, pl.ds(offset, size), :] = dot(vc[pl.ds(offset, size), :], gt[pair])

        def after(pair):
            dsum = d_ref[pair]
            for start in range(0, size, SUB):
                here = pl.ds(offset + start, SUB)
                dsum = dsum + jnp.sum((s_ref[pair, here, :] * dp_ref[pair, here, :]).reshape(tile), axis=0)
            d_ref[pair] = dsum

        staggered(products, after, pairs)

    def value_grads(offset, size, then):
        keys = pl.ds(offset, size)
        dv_acc[keys, :] = jnp.zeros((size, D), F32)
        some = pl.ds(0, size)

        def weights(pair, slot):
            shift = m_ref[pair]
            for start in range(0, size, SUB):
                here = pl.ds(offset + start, SUB)
                p = jnp.exp2(s_ref[pair, here, :] - shift[0:1])
                s_ref[pair, here, :] = p
                to = pl.ds(start, SUB)
                hi, lo = split(p)
                pcat[slot, to, 0 : 2 * rows] = hi
                pcat[slot, to, 2 * rows :] = lo

        def products(pair, slot):
            dv = dot(pcat[slot, some, :], gr[pair])
            dv_acc[keys, :] += dv[:, :D] + dv[:, D:]

        ahead(weights, products, 0, pairs, STEP, then)

    def key_grads(offset, size, first, begin, end):
        keys = pl.ds(offset, size)
        if begin == 0:
            dk_acc[keys, :] = jnp.zeros((size, D), F32)
        some = pl.ds(0, size)

        def weights(pair, slot):
            mean = d_ref[pair][0:1]
            for start in range(0, size, SUB):
                here = pl.ds(offset + start, SUB)
                to = pl.ds(start, SUB)
                hi, lo = split(s_ref[pair, here, :] * (dp_ref[pair, here, :] - mean))
                dcat[slot, to, 0 : 2 * rows] = hi
                dcat[slot, to, 2 * rows :] = lo

        def products(pair, slot):
            dk = dot(dcat[slot, some, :], qr[pair])
            dk_acc[keys, :] += dk[:, :D] + dk[:, D:]
            high = dot(kt[:, keys], dcat[slot, some, 0 : 2 * rows])
            dq = high[:D] + high[D:] + dot(kt[0:D, keys], dcat[slot, some, 2 * rows :])
            if first:
                dqt[pair] = dq
            else:
                dqt[pair] += dq

        ahead(weights, products, begin, end, STEP if (end - begin) % STEP == 0 else 2)

    def lead_queries(begin, end, then):
        keys = pl.ds(0, lead)

        def weights(pair, slot):
            shift, mean = m_ref[pair], d_ref[pair][0:1]
            for start in range(0, lead, SUB):
                here = pl.ds(start, SUB)
                p = jnp.exp2(s_ref[pair, here, :] - shift)
                ds = p * (dp_ref[pair, here, :] - mean)
                s_ref[pair, here, :] = p
                dp_ref[pair, here, :] = ds
                hi, lo = split(ds)
                dcat[slot, here, 0 : 2 * rows] = hi
                dcat[slot, here, 2 * rows :] = lo

        def products(pair, slot):
            high = dot(kt[:, keys], dcat[slot, :, 0 : 2 * rows])
            dq = high[:D] + high[D:] + dot(kt[0:D, keys], dcat[slot, :, 2 * rows :])
            then(pair, dqt[pair] + dq)

        ahead(weights, products, begin, end, 2)

    def lead_grads(then):
        dk_acc[pl.ds(0, lead), :] = jnp.zeros((lead, D), F32)
        dv_acc[pl.ds(0, lead), :] = jnp.zeros((lead, D), F32)

        def weights(pair, slot):
            for start in range(0, lead, SUB):
                here = pl.ds(start, SUB)
                hi, lo = split(s_ref[pair, here, :])
                pcat[slot, here, 0 : 2 * rows] = hi
                pcat[slot, here, 2 * rows :] = lo
                hi, lo = split(dp_ref[pair, here, :])
                dcat[slot, here, 0 : 2 * rows] = hi
                dcat[slot, here, 2 * rows :] = lo

        def products(pair, slot):
            dv = dot(pcat[slot], gr[pair])
            dv_acc[pl.ds(0, lead), :] += dv[:, :D] + dv[:, D:]
            dk = dot(dcat[slot], qr[pair])
            dk_acc[pl.ds(0, lead), :] += dk[:, :D] + dk[:, D:]

        ahead(weights, products, 0, pairs, 2, then)

    every, front, last = range(parts), range(cut), range(cut, parts)
    loops = pairs // STEP
    assert cut - 1 <= pairs // 2 and parts > 2 * loops

    staggered(
        lead_products,
        lambda pair: sums(pair, 0, lead, True),
        STEP,
        lambda i: relay(0, [i]),
    )
    relay(0, range(loops, cut))
    place_keys(kv2.at[0], 0, off2, front_size)
    key_scores(off2, front_size)
    relay(0, range(max(loops, cut), parts))
    place_keys(kv2.at[0], last_at, off2 + last_at, last_size)
    key_scores(off2 + last_at, last_size)
    arrive(0, front)
    place_keys(kv1.at[0], 0, off1, front_size)
    key_scores(off1, front_size)
    relay(1, range(1))
    arrive(0, last)
    place_keys(kv1.at[0], last_at, off1 + last_at, last_size)
    key_scores(off1 + last_at, last_size)

    def total(pair, carry):
        l = jnp.sum(l_ref[pair], axis=0, keepdims=True)
        d_ref[pair] = d_ref[pair] / l
        m_ref[pair] = m_ref[pair] + jnp.log2(l)
        return carry

    lax.fori_loop(0, pairs, total, 0)

    acc = (dk_acc, dv_acc)

    def out_y(i, t):
        return remote(
            acc[t].at[pl.ds(off1 + i * SUB, SUB)], ry.at[t, pl.ds(i * SUB, SUB)],
            out_y_send.at[i, t], out_y_recv.at[i, t], (partner, head),
        )

    def out_z(i, t):
        return remote(
            acc[t].at[pl.ds(off2 + i * SUB, SUB)], rz.at[t, pl.ds(i * SUB, SUB)],
            out_z_send.at[i, t], out_z_recv.at[i, t], (above, head),
        )

    def send_y(t, some, when=True):
        @pl.when(when)
        def _():
            for i in some:
                out_y(i, t).start()

    def send_z_odd(t, some):
        @pl.when(odd)
        def _():
            for i in some:
                out_z(i, t).start()

    def join(t, some):
        for i in some:
            out_y(i, t).wait_recv()

            @pl.when(even)
            def _():
                acc[t][pl.ds(off2 + i * SUB, SUB), :] += ry[t, pl.ds(i * SUB, SUB), :]
                out_z(i, t).start()

    width = heads * D
    share = rows // n_head

    def to_peer(step, pair):
        other = lax.rem(head + step, n_head)
        return remote(
            dqs.at[pair, pl.ds(other * share, share), :],
            gq_ref.at[:, pl.ds(pl.multiple_of(head * width + pair * 2 * D, D), 2 * D)],
            q_send.at[step - 1, pair], q_recv.at[step - 1, pair], (seq, other),
        )

    def keep(pair):
        return pltpu.make_async_copy(
            dqs.at[pair, pl.ds(head * share, share), :],
            gq_ref.at[:, pl.ds(pl.multiple_of(head * width + pair * 2 * D, D), 2 * D)],
            q_local.at[pair],
        )

    def stage(pair, dq):
        for half in range(2):
            dqs[pair, :, half * D : (half + 1) * D] = dq[:, half * rows : (half + 1) * rows].T * factor
        for step in range(1, n_head):
            to_peer(step, pair).start()
        keep(pair).start()

    value_grads(off1, block, lambda i: relay(1, [1 + i]))
    send_y(1, every, odd)
    value_grads(off2, block, lambda i: relay(1, [1 + loops + i]))
    relay(1, range(1 + 2 * loops, parts))
    send_y(1, every, even)
    send_z_odd(1, every)
    place_values(kv2.at[1], 0, off2, block)
    value_scores(off2, block)
    arrive(1, front)
    place_values(kv1.at[1], 0, off1, front_size)
    value_scores(off1, front_size)
    arrive(1, last)
    place_values(kv1.at[1], last_at, off1 + last_at, last_size)
    value_scores(off1 + last_at, last_size)

    def settle_mean(pair, carry):
        d_ref[pair] = jnp.broadcast_to(jnp.sum(d_ref[pair], axis=0, keepdims=True), (8, 2 * rows))
        return carry

    lax.fori_loop(0, pairs, settle_mean, 0)

    quarter = pairs // 4
    key_grads(off1 + last_at, last_size, True, 0, pairs)
    send_y(0, last)
    join(1, range(1))
    key_grads(off1, front_size, False, 0, quarter)
    key_grads(off2, block, False, 0, quarter)
    lead_queries(0, quarter, stage)
    join(1, range(1, 3))
    key_grads(off1, front_size, False, quarter, pairs)
    send_y(0, front)
    join(1, range(3, parts))
    key_grads(off2, block, False, quarter, pairs)
    send_z_odd(0, every)
    join(0, last)
    lead_queries(quarter, pairs, stage)
    join(0, range(1))

    def join_front(i):
        @pl.when(i < cut - 1)
        def _():
            join(0, [i + 1])

    lead_grads(join_front)
    grk_ref[...] = dk_acc[pl.ds(block, rows), :]
    grv_ref[...] = dv_acc[pl.ds(block, rows), :]

    @pl.when(odd)
    def _():
        for t in range(2):
            acc[t][pl.ds(0, block), :] += ry[t]

    out = (gpk_ref, gpv_ref)
    for t in (1, 0):
        for i in every:
            here = pl.ds(i * SUB, SUB)
            out_z(i, t).wait_recv()
            out[t][here, :] = acc[t][here, :] + rz[t, here, :]

    for pair in range(pairs):
        keep(pair).wait()
        for step in range(1, n_head):
            to_peer(step, pair).wait()
    for i, t in pieces:
        in_z(i, t).wait_send()
        in_y_own(i, t).wait_send()
        out_y(i, t).wait_send()
        out_z(i, t).wait_send()


def settle(*refs):
    count = (len(refs) - 1) // 2
    store_sem = refs[-1]
    stores = [
        pltpu.make_async_copy(refs[i], refs[count + i], store_sem.at[i]) for i in range(count)
    ]
    for store in stores:
        store.start()
    for store in stores:
        store.wait()


def per_device(n_seq, n_head, queries, prefix_keys, prefix_value_rows, response_keys, response_values, out_grad, lengths):
    rows, width = queries.shape
    block = prefix_keys.shape[0]
    assert prefix_keys.shape[1] == D
    heads = width // D
    pairs = heads // 2
    keys = WINDOW * block + rows
    lead = block + rows
    vmem = pl.BlockSpec(memory_space=pltpu.VMEM)
    anywhere = pl.BlockSpec(memory_space=pl.ANY)
    part_sems = pltpu.SemaphoreType.DMA((block // SUB, 2))
    shape = jax.ShapeDtypeStruct
    results = pl.pallas_call(
        functools.partial(kernel, n_seq, n_head),
        out_shape=(
            pltpu.VMEM((rows // n_head, width * n_head), F32),
            pltpu.VMEM((block, D), F32),
            pltpu.VMEM((block, D), F32),
            pltpu.VMEM((rows, D), F32),
            pltpu.VMEM((rows, D), F32),
        ),
        in_specs=[pl.BlockSpec(memory_space=pltpu.SMEM)] + [anywhere] * 6,
        out_specs=(vmem,) * 5,
        scratch_shapes=[
            pltpu.VMEM((rows, width), F32),
            pltpu.VMEM((rows, width), F32),
            pltpu.VMEM((2, block, D), F32),
            pltpu.VMEM((2, block, D), F32),
            pltpu.VMEM((2, block, D), F32),
            pltpu.VMEM((2, rows, D), F32),
            pltpu.VMEM((keys, 3 * D), BF16),
            pltpu.VMEM((keys, 3 * D), BF16),
            pltpu.VMEM((2 * D, keys), BF16),
            pltpu.VMEM((pairs, 3 * D, 2 * rows), BF16),
            pltpu.VMEM((pairs, 3 * D, 2 * rows), BF16),
            pltpu.VMEM((pairs, 4 * rows, 2 * D), BF16),
            pltpu.VMEM((pairs, 4 * rows, 2 * D), BF16),
            pltpu.VMEM((pairs, keys, 2 * rows), F32),
            pltpu.VMEM((pairs, keys, 2 * rows), F32),
            pltpu.VMEM((pairs, 1, 2 * rows), F32),
            pltpu.VMEM((pairs, 8, 2 * rows), F32),
            pltpu.VMEM((pairs, 8, 2 * rows), F32),
            pltpu.VMEM((2, lead, 4 * rows), BF16),
            pltpu.VMEM((2, lead, 4 * rows), BF16),
            pltpu.VMEM((keys, D), F32),
            pltpu.VMEM((keys, D), F32),
            pltpu.VMEM((pairs, D, 2 * rows), F32),
            pltpu.VMEM((pairs, rows, 2 * D), F32),
            pltpu.VMEM((2, block, D), F32),
            pltpu.VMEM((2, block, D), F32),
        ]
        + [part_sems] * 8
        + [pltpu.SemaphoreType.DMA((n_head - 1, pairs))] * 2
        + [pltpu.SemaphoreType.DMA((pairs,)), pltpu.SemaphoreType.DMA((6,))],
        compiler_params=pltpu.CompilerParams(
            collective_id=0, has_side_effects=True, vmem_limit_bytes=65000000
        ),
    )(lengths, queries, prefix_keys, prefix_value_rows, response_keys, response_values, out_grad)
    return pl.pallas_call(
        settle,
        out_shape=tuple(shape(x.shape, x.dtype) for x in results),
        in_specs=[vmem] * len(results),
        out_specs=(anywhere,) * len(results),
        scratch_shapes=[pltpu.SemaphoreType.DMA((len(results),))],
        compiler_params=pltpu.CompilerParams(vmem_limit_bytes=8 * 1024 * 1024),
    )(*(pltpu.with_memory_space_constraint(x, pltpu.VMEM) for x in results))


def solution(mesh):
    sharded = P("seq", "head")
    return jax.shard_map(
        functools.partial(per_device, mesh.shape["seq"], mesh.shape["head"]),
        mesh=mesh,
        in_specs=(sharded,) * 6 + (P("seq"),),
        out_specs=(P(("seq", "head"), None),) + (sharded,) * 4,
        check_vma=False,
    )
```
